32 devices in a mesh: row: 8 (over z, core), col: 4 (over y, x).
Axes of the slice: x: 2, y: 2, z: 4, core: 2. Of those that a mesh axis runs over, the one named last changes fastest.
Arguments:
- velocity: float32 [3, 64, 64, 64], P(None, 'row', 'col'), may hold values from -6 to 6
Outputs:
- advanced: float32 [3, 64, 64, 64], P(None, 'row', 'col')
The draws below stay inside these ranges and needn't reach their ends.
All inputs are finite; a program needn't handle non-finite values.
Results may differ from the reference program's by a relative error of at most 0.0003.
Values sent between devices are 32-bit elements.
A program may use at most 64 MiB of HBM per device.

```python
import jax
import jax.numpy as jnp

N = 64


def block_levels(key, shape, pieces, least, top_value):
    loudness = 1.0
    for axis_at, shards_of in pieces:
        draws = jax.random.uniform(jax.random.fold_in(jax.random.fold_in(key, 6), axis_at), (shards_of,), jnp.float32, least / len(pieces), top_value / len(pieces))
        loudness = loudness * jnp.repeat(jnp.exp(draws), shape[axis_at] // shards_of).reshape((-1,) + (1,) * (len(shape) - 1 - axis_at))
    return loudness


def scatter_about(key, extent, deviation, bound, shards=(), held_as=jnp.bfloat16):
    loudness = block_levels(key, extent, shards, -0.22, 0.18) if shards else 1.0
    array = jax.random.normal(key, extent, jnp.float32) * deviation * loudness
    return jnp.minimum(jnp.maximum(array, -bound), bound).astype(held_as)


def setup_inputs(seed: int = 0) -> dict:
    arg_keys = jax.random.split(jax.random.key(seed), 2)
    return {
        "velocity": scatter_about(arg_keys[0], (3, N, N, N), 1.0, 6.0, ((1, 8), (2, 4)), jnp.float32),
    }


def spectrum(field):
    return jnp.fft.rfftn(field, axes=(1, 2, 3), norm="forward")[..., : N // 2]


def grid_field(spectral):
    nyquist = jnp.zeros(spectral.shape[:3] + (1,), spectral.dtype)
    padded = jnp.concatenate([spectral, nyquist], axis=3)
    return jnp.fft.irfftn(padded, s=(N, N, N), axes=(1, 2, 3), norm="forward")


def wave_numbers():
    index = jnp.arange(N, dtype=jnp.int32)
    signed = jnp.where(index < N // 2, index, index - N)
    half = jnp.arange(N // 2, dtype=jnp.int32)
    return signed[:, None, None], signed[None, :, None], half[None, None, :]


def cross_with(left, right):
    return jnp.stack([left[1] * right[2] - left[2] * right[1], left[2] * right[0] - left[0] * right[2], left[0] * right[1] - left[1] * right[0]])


def reference(velocity):
    int_waves = wave_numbers()
    mask = ((3 * jnp.abs(int_waves[0]) < N) & (3 * jnp.abs(int_waves[1]) < N) & (3 * jnp.abs(int_waves[2]) < N)).astype(jnp.float32)
    waves = [wave.astype(jnp.float32) for wave in int_waves]
    squared = waves[0] * waves[0] + waves[1] * waves[1] + waves[2] * waves[2]
    safe_norm = jnp.where(squared > 0, squared, jnp.float32(1.0))
    viscous = squared / N
    step = 2.0 / N

    def project(field):
        along = (waves[0] * field[0] + waves[1] * field[1] + waves[2] * field[2]) / safe_norm
        return field - jnp.stack([waves[0] * along, waves[1] * along, waves[2] * along])

    def tendency(state):
        flow = grid_field(state)
        spin = grid_field(1j * cross_with(waves, state))
        product = cross_with(flow, spin)
        return project(mask * spectrum(product)) - viscous * state

    start = project(mask * spectrum(velocity))
    first = tendency(start)
    second = tendency(start + step * first)
    return grid_field(start + 0.5 * step * (first + second)).astype(jnp.float32)
```

```python
import jax
import jax.numpy as jnp
import numpy as np
from jax import lax
from jax.sharding import PartitionSpec as P

precision = lax.Precision.HIGH


def band_waves(points, shards, half):
    top = (points - 1) // 3
    if half:
        width = -(-(top + 1) // shards) * shards
        return np.arange(width)
    width = -(-(2 * top + 1) // shards) * shards
    index = np.arange(width)
    return np.where(index <= width // 2, index, index - width)


def rotation(points, waves, sign):
    turns = (np.arange(points)[:, None] * waves[None, :]) % points
    angle = turns * (2.0 * np.pi / points)
    cosine, sine = np.cos(angle), sign * np.sin(angle)
    return np.stack([np.stack([cosine, sine], -1), np.stack([-sine, cosine], -1)], -2)


def cross_with(left, right):
    return jnp.stack(
        [
            left[1] * right[2] - left[2] * right[1],
            left[2] * right[0] - left[0] * right[2],
            left[0] * right[1] - left[1] * right[0],
        ]
    )


def local(velocity):
    points = velocity.shape[3]
    rows, cols = lax.axis_size("row"), lax.axis_size("col")
    kz_all, ky_all = band_waves(points, cols, True), band_waves(points, rows, False)
    kx_all = band_waves(points, 8, False)
    nz, ny = len(kz_all) // cols, len(ky_all) // rows
    px, py = points // rows, points // cols
    f32 = lambda a: jnp.asarray(a.astype(np.float32))

    fwd = [rotation(points, k, -1.0) / points for k in (kx_all, ky_all, kz_all)]
    inv = [rotation(points, k, 1.0) for k in (kx_all, ky_all, kz_all)]
    weight = np.where(kz_all == 0, 1.0, 2.0)
    z_fwd = f32(fwd[2][:, :, 0, :].reshape(points, cols, nz, 2))
    z_inv = f32((inv[2][:, :, :, 0] * weight[None, :, None]).reshape(points, cols, nz, 2))
    y_fwd = f32(fwd[1].reshape(cols, py, rows, ny, 2, 2))
    y_inv = f32(inv[1].reshape(cols, py, rows, ny, 2, 2))
    x_fwd = f32(fwd[0].reshape(rows, px, len(kx_all), 2, 2))
    x_inv = f32(inv[0].reshape(rows, px, len(kx_all), 2, 2))

    kx = f32(kx_all)[None, None, :]
    ky = lax.dynamic_slice_in_dim(f32(ky_all), lax.axis_index("row") * ny, ny)[None, :, None]
    kz = lax.dynamic_slice_in_dim(f32(kz_all), lax.axis_index("col") * nz, nz)[:, None, None]
    kept = (3 * jnp.abs(kx) < points) & (3 * jnp.abs(ky) < points) & (3 * jnp.abs(kz) < points)
    squared = kx * kx + ky * ky + kz * kz
    safe_norm = jnp.where(squared > 0, squared, 1.0)
    viscous = squared / points

    def dot(spec, a, b):
        return jnp.einsum(spec, a, b, precision=precision)

    def swap(a, axis):
        return lax.all_to_all(a, axis, split_axis=0, concat_axis=0)

    def spectra(field):
        a = swap(dot("cpqr,rnsj->njcpqs", field, z_fwd), "col")
        a = swap(dot("micpqs,mqntij->njcpst", a, y_fwd), "row")
        return dot("micpst,mpkij->jcstk", a, x_fwd)

    def grids(spectral):
        a = swap(dot("icstk,npkij->njcpst", spectral, x_inv), "row")
        a = swap(dot("micpst,nqmtij->njcpqs", a, y_inv), "col")
        return dot("micpqs,rmsi->cpqr", a, z_inv)

    def project(b):
        b = jnp.where(kept, b, 0.0)
        along = (kx * b[:, 0] + ky * b[:, 1] + kz * b[:, 2]) / safe_norm
        return b - jnp.stack([kx * along, ky * along, kz * along], 1)

    def tendency(state):
        waves = (kx, ky, kz)
        curl = jnp.stack([-cross_with(waves, state[1]), cross_with(waves, state[0])])
        joined = grids(jnp.concatenate([state, curl], 1))
        return project(spectra(cross_with(joined[:3], joined[3:]))) - viscous * state

    start = project(spectra(velocity))
    step = 2.0 / points
    first = tendency(start)
    second = tendency(start + step * first)
    return grids(start + 0.5 * step * (first + second))


def solution(mesh):
    placed = P(None, "row", "col", None)
    return jax.shard_map(local, mesh=mesh, in_specs=(placed,), out_specs=placed, check_vma=False)
```

```python
import functools

import jax
import jax.numpy as jnp
import ml_dtypes
import numpy as np
from jax import lax
from jax.experimental import pallas as pl
from jax.experimental.pallas import tpu as pltpu
from jax.sharding import PartitionSpec as P

MESH = pl.DeviceIdType.MESH
PAD = 8


def band_waves(points, shards, half, pad):
    top = (points - 1) // 3
    kept = np.arange(top + 1) if half else np.concatenate([np.arange(top + 1), np.arange(-top, 0)])
    each = -(-len(kept) // shards)
    pad = -(-each // pad) * pad
    table = np.full((shards * each,), points)
    table[: len(kept)] = kept
    out = np.full((shards, pad), points)
    out[:, :each] = table.reshape(shards, each)
    return out


def circle(points, waves):
    x = np.arange(points).reshape((-1,) + (1,) * waves.ndim)
    angle = ((x * waves) % points) * (2.0 * np.pi / points)
    real = (waves < points).astype(np.float64)
    return np.cos(angle) * real, np.sin(angle) * real


def halves(table):
    high = table.astype(np.float32).astype(ml_dtypes.bfloat16)
    low = (table - high.astype(np.float64)).astype(np.float32).astype(ml_dtypes.bfloat16)
    return np.stack([high, low])


def tables(points, rows, cols):
    kz = band_waves(points, cols, True, PAD)
    ky = band_waves(points, rows, False, PAD)
    kx = band_waves(points, 1, False, 16)[0]
    px, py = points // rows, points // cols
    cz, sz = circle(points, kz)
    zf = np.stack([cz, -sz], 2).transpose(1, 2, 3, 0).reshape(-1, points) / points
    weight = np.where(kz == 0, 1.0, 2.0)[None, :, None, :]
    zi = (np.stack([cz, -sz], 2) * weight).reshape(points, -1)

    def kron(spec, parts, eye, left, scale):
        made = [np.einsum(spec, part, np.eye(eye)).reshape(left, -1) * scale for part in parts]
        return np.concatenate(made, 1)

    cy = [a.reshape(cols, py, rows, PAD) for a in circle(points, ky)]
    cx = [a.reshape(rows, px, len(kx)) for a in circle(points, kx)]
    yf = kron("qyrt,xX->qxyrXt", cy, px, points * px, 1 / points)
    yi = kron("qyrt,xX->rxtqXy", cy, px, rows * px * PAD, 1.0)
    xf = kron("rxk,tT->rxtkT", cx, PAD, points * PAD, 1 / points)
    xi = kron("rxk,tT->ktrxT", cx, PAD, len(kx) * PAD, 1.0)
    lanes = len(kx) * PAD
    wx = np.broadcast_to(np.repeat(kx, PAD)[None, :], (PAD, lanes))
    wy = np.broadcast_to(np.tile(ky[:, None, None, :], (1, 1, len(kx), 1)).reshape(rows, 1, lanes), (rows, PAD, lanes))
    wz = np.broadcast_to(kz[:, :, None], (cols, PAD, lanes))
    waves = [np.ascontiguousarray(w).astype(np.float32) for w in (wx, wy, wz)]
    return [halves(t) for t in (zf, zi, yf, yi, xf, xi)] + waves


def dot(a, b, transposed=False):
    dims = (((1,), (1 if transposed else 0,)), ((), ()))
    return lax.dot_general(a, b, dims, preferred_element_type=jnp.float32)


def split(x):
    high = x.astype(jnp.bfloat16)
    return high, (x - high.astype(jnp.float32)).astype(jnp.bfloat16)


def dot_left(table, x, transposed=False):
    high, low = split(x)
    return dot(table[0], high, transposed) + (dot(table[0], low, transposed) + dot(table[1], high, transposed))


def dot_right(x, table):
    high, low = split(x)
    return dot(high, table[0]) + (dot(low, table[0]) + dot(high, table[1]))


def turn(re, im, table, sign):
    n, half = re.shape[0], table.shape[2] // 2
    out = dot_right(jnp.concatenate([re, im], 0), table)
    re_c, re_s, im_c, im_s = out[:n, :half], out[:n, half:], out[n:, :half], out[n:, half:]
    if sign > 0:
        return re_c - im_s, im_c + re_s
    return re_c + im_s, im_c - re_s


def cross(a, b):
    return [a[1] * b[2] - a[2] * b[1], a[2] * b[0] - a[0] * b[2], a[0] * b[1] - a[1] * b[0]]


def kernel(points, rows, cols, counts, v_ref, zf, zi, yf, yi, xf, xi, wx, wy, wz, out_ref, *scratch):
    row, col = lax.axis_index("row"), lax.axis_index("col")
    px, py = points // rows, points // cols
    cell, tile = px * py, 2 * px * PAD
    peers = {"row": (row, rows), "col": (col, cols)}
    exchanges = len(counts)
    sends, lands = scratch[:exchanges], scratch[exchanges : 2 * exchanges]
    send_sems, land_sems = scratch[2 * exchanges : 3 * exchanges], scratch[3 * exchanges :]

    barrier = pltpu.get_barrier_semaphore()
    for axis, (me, n) in peers.items():
        for d in range(1, n):
            pl.semaphore_signal(barrier, inc=1, device_id={axis: lax.rem(me + d, n)}, device_id_type=MESH)
    pl.semaphore_wait(barrier, rows + cols - 2)

    def swap(at, blocks):
        axis = counts[at]
        me, n = peers[axis]
        send, land = sends[at], lands[at]
        for j in range(n):
            send[j] = blocks[j]
        copies = []
        for d in range(1, n):
            to = lax.rem(me + d, n)
            copy = pltpu.make_async_remote_copy(
                src_ref=send.at[to], dst_ref=land.at[me], send_sem=send_sems[at].at[d - 1],
                recv_sem=land_sems[at].at[d - 1], device_id={axis: to}, device_id_type=MESH)
            copy.start()
            copies.append(copy)
        land[me] = send[me]
        for copy in copies:
            copy.wait()
        return [land[j] for j in range(n)]

    lane = lax.broadcasted_iota(jnp.int32, (1, tile), 1) < tile // 2
    flip = lambda a: pltpu.roll(a, tile // 2, 1)

    def weave(re, im):
        blocks = []
        for j in range(re.shape[1] // tile):
            a, b = re[:, j * tile : (j + 1) * tile], im[:, j * tile : (j + 1) * tile]
            blocks += [jnp.where(lane, a, flip(b)), jnp.where(lane, flip(a), b)]
        return blocks

    def unweave(blocks):
        re, im = [], []
        for a, b in zip(blocks[::2], blocks[1::2]):
            re.append(jnp.where(lane, a, flip(b)))
            im.append(jnp.where(lane, flip(a), b))
        return jnp.concatenate(re, 1), jnp.concatenate(im, 1)

    def spectra(at, lines):
        deep = 2 * PAD
        got = swap(at, [lines[p * deep : (p + 1) * deep] for p in range(cols)])
        pair = []
        for part in range(2):
            stacks = [
                jnp.concatenate([g[part * PAD : (part + 1) * PAD, c * cell : (c + 1) * cell] for c in range(3)], 0)
                for g in got
            ]
            pair.append(jnp.concatenate(stacks, 1))
        got = swap(at + 1, weave(*turn(*pair, yf, -1)))
        return turn(*unweave(got), xf, -1)

    def grids(at, re, im):
        n = re.shape[0] // PAD
        got = swap(at, weave(*turn(re, im, xi, 1)))
        re, im = turn(*unweave(got), yi, 1)
        got = swap(at + 1, [
            jnp.concatenate([re[:, q * cell : (q + 1) * cell], im[:, q * cell : (q + 1) * cell]], 1)
            for q in range(cols)])
        stacks = []
        for c in range(n):
            parts = [g[c * PAD : (c + 1) * PAD, p * cell : (p + 1) * cell] for g in got for p in range(2)]
            stacks.append(jnp.concatenate(parts, 0))
        return dot_left(zi, jnp.concatenate(stacks, 1))

    waves = (wx[...], wy[row], wz[col])
    kept = functools.reduce(jnp.logical_and, [3.0 * jnp.abs(w) < points for w in waves])
    squared = waves[0] * waves[0] + waves[1] * waves[1] + waves[2] * waves[2]
    safe_norm = jnp.where(squared > 0, squared, 1.0)
    viscous = squared * (1.0 / points)

    def project(b):
        b = [jnp.where(kept, b[c * PAD : (c + 1) * PAD], 0.0) for c in range(3)]
        along = (waves[0] * b[0] + waves[1] * b[1] + waves[2] * b[2]) / safe_norm
        return [b[c] - waves[c] * along for c in range(3)]

    def tendency(at, re, im):
        joined = grids(
            at,
            jnp.concatenate(re + [-w for w in cross(waves, im)], 0),
            jnp.concatenate(im + cross(waves, re), 0))
        fields = [joined[:, c * cell : (c + 1) * cell] for c in range(6)]
        product = jnp.concatenate(cross(fields[:3], fields[3:]), 1)
        b_re, b_im = spectra(at + 2, dot_left(zf, product))
        return (
            [b - viscous * a for b, a in zip(project(b_re), re)],
            [b - viscous * a for b, a in zip(project(b_im), im)],
        )

    b_re, b_im = spectra(0, dot_left(zf, v_ref[...], transposed=True))
    re, im = project(b_re), project(b_im)
    step = 2.0 / points
    r1_re, r1_im = tendency(2, re, im)
    mid_re = [a + step * r for a, r in zip(re, r1_re)]
    mid_im = [a + step * r for a, r in zip(im, r1_im)]
    r2_re, r2_im = tendency(6, mid_re, mid_im)
    end_re = [a + 0.5 * step * (r + s) for a, r, s in zip(re, r1_re, r2_re)]
    end_im = [a + 0.5 * step * (r + s) for a, r, s in zip(im, r1_im, r2_im)]
    out_ref[...] = grids(10, jnp.concatenate(end_re, 0), jnp.concatenate(end_im, 0))


def solution(mesh):
    rows, cols = mesh.shape["row"], mesh.shape["col"]

    def local(velocity):
        points = velocity.shape[3]
        px, py = points // rows, points // cols
        cell, tile = px * py, 2 * px * PAD
        consts = tables(points, rows, cols)
        forward = [(cols, 2 * PAD, 3 * cell), (rows, 3 * PAD, tile)]
        inverse = lambda n: [(rows, n * PAD, tile), (cols, n * PAD, 2 * cell)]
        shapes = forward + 2 * (inverse(6) + forward) + inverse(3)
        axes = ["col", "row"] + 2 * ["row", "col", "col", "row"] + ["row", "col"]
        sems = [pltpu.SemaphoreType.DMA(((rows if a == "row" else cols) - 1,)) for a in axes]
        buffers = [pltpu.VMEM(s, jnp.float32) for s in shapes]
        out = pl.pallas_call(
            functools.partial(kernel, points, rows, cols, axes),
            out_shape=jax.ShapeDtypeStruct((points, 3 * cell), jnp.float32),
            in_specs=[pl.BlockSpec(memory_space=pltpu.VMEM)] * (1 + len(consts)),
            out_specs=pl.BlockSpec(memory_space=pltpu.VMEM),
            scratch_shapes=buffers + buffers + sems + sems,
            compiler_params=pltpu.CompilerParams(
                collective_id=0, has_side_effects=True, vmem_limit_bytes=60 * 1024 * 1024),
        )(velocity.reshape(3 * cell, points), *[jnp.asarray(c) for c in consts])
        return out.reshape(points, 3, px, py).transpose(1, 2, 3, 0)

    placed = P(None, "row", "col", None)
    return jax.shard_map(local, mesh=mesh, in_specs=(placed,), out_specs=placed, check_vma=False)
```

```python
import functools

import jax
import jax.numpy as jnp
import ml_dtypes
import numpy as np
from jax import lax
from jax.experimental import pallas as pl
from jax.experimental.pallas import tpu as pltpu
from jax.sharding import PartitionSpec as P

MESH = pl.DeviceIdType.MESH
PAD = 8


def band_waves(points, shards, half, pad):
    top = (points - 1) // 3
    kept = np.arange(top + 1) if half else np.concatenate([np.arange(top + 1), np.arange(-top, 0)])
    each = -(-len(kept) // shards)
    pad = -(-each // pad) * pad
    table = np.full((shards * each,), points)
    table[: len(kept)] = kept
    out = np.full((shards, pad), points)
    out[:, :each] = table.reshape(shards, each)
    return out


def circle(points, waves):
    x = np.arange(points).reshape((-1,) + (1,) * waves.ndim)
    angle = ((x * waves) % points) * (2.0 * np.pi / points)
    real = (waves < points).astype(np.float64)
    return np.cos(angle) * real, np.sin(angle) * real


def halves(table):
    high = table.astype(np.float32).astype(ml_dtypes.bfloat16)
    low = (table - high.astype(np.float64)).astype(np.float32).astype(ml_dtypes.bfloat16)
    return np.stack([high, low])


def tables(points, rows, cols):
    kz = band_waves(points, cols, True, PAD)
    ky = band_waves(points, rows, False, PAD)
    kx = band_waves(points, 1, False, 16)[0]
    px, py = points // rows, points // cols
    cz, sz = circle(points, kz)
    zf = np.stack([cz, -sz], 2).transpose(1, 2, 3, 0).reshape(-1, points) / points
    weight = np.where(kz == 0, 1.0, 2.0)[None, :, None, :]
    zi = (np.stack([cz, -sz], 2) * weight).reshape(points, -1)

    def kron(spec, parts, eye, left, scale):
        made = [np.einsum(spec, part, np.eye(eye)).reshape(left, -1) * scale for part in parts]
        return np.concatenate(made, 1)

    cy = [a.reshape(cols, py, rows, PAD) for a in circle(points, ky)]
    cx = [a.reshape(rows, px, len(kx)) for a in circle(points, kx)]
    yf = kron("qyrt,xX->qxyrXt", cy, px, points * px, 1 / points)
    yi = kron("qyrt,xX->rxtqXy", cy, px, rows * px * PAD, 1.0)
    xf = kron("rxk,tT->rxtkT", cx, PAD, points * PAD, 1 / points)
    xi = kron("rxk,tT->ktrxT", cx, PAD, len(kx) * PAD, 1.0)
    lanes = len(kx) * PAD
    wx = np.broadcast_to(np.repeat(kx, PAD)[None, :], (PAD, lanes))
    wy = np.broadcast_to(np.tile(ky[:, None, None, :], (1, 1, len(kx), 1)).reshape(rows, 1, lanes), (rows, PAD, lanes))
    wz = np.broadcast_to(kz[:, :, None], (cols, PAD, lanes))
    wt = np.broadcast_to(ky[:, None, :], (rows, px, PAD)).reshape(1, -1)
    waves = [np.ascontiguousarray(w).astype(np.float32) for w in (wx, wy, wz, wt)]
    return [halves(t) for t in (zf, zi, yf, yi, xf, xi)] + waves


def dot(a, b, transposed=False):
    dims = (((1,), (1 if transposed else 0,)), ((), ()))
    return lax.dot_general(a, b, dims, preferred_element_type=jnp.float32)


def split(x):
    high = x.astype(jnp.bfloat16)
    return high, (x - high.astype(jnp.float32)).astype(jnp.bfloat16)


def dot_left(table, x, transposed=False):
    high, low = split(x)
    return dot(table[0], high, transposed) + (dot(table[0], low, transposed) + dot(table[1], high, transposed))


def dot_right(x, table):
    high, low = split(x)
    return dot(high, table[0]) + (dot(low, table[0]) + dot(high, table[1]))


def turn(re, im, table, sign):
    n, half = re.shape[0], table.shape[2] // 2
    out = dot_right(jnp.concatenate([re, im], 0), table)
    re_c, re_s, im_c, im_s = out[:n, :half], out[:n, half:], out[n:, :half], out[n:, half:]
    if sign > 0:
        return re_c - im_s, im_c + re_s
    return re_c + im_s, im_c - re_s


def cross(a, b):
    return [a[1] * b[2] - a[2] * b[1], a[2] * b[0] - a[0] * b[2], a[0] * b[1] - a[1] * b[0]]


def kernel(points, rows, cols, counts, v_ref, zf, zi, yf, yi, xf, xi, wx, wy, wz, wt, out_ref, *scratch):
    row, col = lax.axis_index("row"), lax.axis_index("col")
    px, py = points // rows, points // cols
    cell, tile = px * py, 2 * px * PAD
    peers = {"row": (row, rows), "col": (col, cols)}
    exchanges = len(counts)
    sends, lands = scratch[:exchanges], scratch[exchanges : 2 * exchanges]
    send_sems, land_sems = scratch[2 * exchanges : 3 * exchanges], scratch[3 * exchanges : 4 * exchanges]
    held = scratch[4 * exchanges : 4 * exchanges + 4]
    loads = [
        pltpu.make_async_copy(source, target, scratch[-1].at[i])
        for i, (source, target) in enumerate(zip((yf, xf, xi, yi), held))
    ]
    for load in loads:
        load.start()
    pending = list(range(4))

    def weights(i):
        if i in pending:
            pending.remove(i)
            loads[i].wait()
        return held[i]

    barrier = pltpu.get_barrier_semaphore()
    for axis, (me, n) in peers.items():
        for d in range(1, n):
            pl.semaphore_signal(barrier, inc=1, device_id={axis: lax.rem(me + d, n)}, device_id_type=MESH)
    pl.semaphore_wait(barrier, rows + cols - 2)

    def swap(at, blocks):
        axis = counts[at]
        me, n = peers[axis]
        send, land = sends[at], lands[at]
        for j in range(n):
            send[j] = blocks[j]
        copies = []
        for d in range(1, n):
            to = lax.rem(me + d, n)
            copy = pltpu.make_async_remote_copy(
                src_ref=send.at[to], dst_ref=land.at[me], send_sem=send_sems[at].at[d - 1],
                recv_sem=land_sems[at].at[d - 1], device_id={axis: to}, device_id_type=MESH)
            copy.start()
            copies.append(copy)
        land[me] = send[me]
        for copy in copies:
            copy.wait()
        return [land[j] for j in range(n)]

    lane = lax.broadcasted_iota(jnp.int32, (1, tile), 1) < tile // 2
    flip = lambda a: pltpu.roll(a, tile // 2, 1)

    def weave(re, im):
        blocks = []
        for j in range(re.shape[1] // tile):
            a, b = re[:, j * tile : (j + 1) * tile], im[:, j * tile : (j + 1) * tile]
            blocks += [jnp.where(lane, a, flip(b)), jnp.where(lane, flip(a), b)]
        return blocks

    def unweave(blocks):
        re, im = [], []
        for a, b in zip(blocks[::2], blocks[1::2]):
            re.append(jnp.where(lane, a, flip(b)))
            im.append(jnp.where(lane, flip(a), b))
        return jnp.concatenate(re, 1), jnp.concatenate(im, 1)

    def spectra(at, lines):
        deep = 2 * PAD
        got = swap(at, [lines[p * deep : (p + 1) * deep] for p in range(cols)])
        pair = []
        for part in range(2):
            stacks = [
                jnp.concatenate([g[part * PAD : (part + 1) * PAD, c * cell : (c + 1) * cell] for c in range(3)], 0)
                for g in got
            ]
            pair.append(jnp.concatenate(stacks, 1))
        got = swap(at + 1, weave(*turn(*pair, weights(0), -1)))
        return turn(*unweave(got), weights(1), -1)

    def grids(at, re, im):
        got = swap(at, weave(*turn(re, im, weights(2), 1)))
        re, im = unweave(got)
        if re.shape[0] == 5 * PAD:
            uy, uz = slice(PAD, 2 * PAD), slice(2 * PAD, 3 * PAD)
            ky, kz = wt[...], wz[col][:, :1]
            spin_re, spin_im = kz * im[uy] - ky * im[uz], ky * re[uz] - kz * re[uy]
            re = jnp.concatenate([re[: 3 * PAD], spin_re, re[3 * PAD :]], 0)
            im = jnp.concatenate([im[: 3 * PAD], spin_im, im[3 * PAD :]], 0)
        n = re.shape[0] // PAD
        re, im = turn(re, im, weights(3), 1)
        got = swap(at + 1, [
            jnp.concatenate([re[:, q * cell : (q + 1) * cell], im[:, q * cell : (q + 1) * cell]], 1)
            for q in range(cols)])
        stacks = []
        for c in range(n):
            parts = [g[c * PAD : (c + 1) * PAD, p * cell : (p + 1) * cell] for g in got for p in range(2)]
            stacks.append(jnp.concatenate(parts, 0))
        return dot_left(zi, jnp.concatenate(stacks, 1))

    waves = (wx[...], wy[row], wz[col])
    kept = functools.reduce(jnp.logical_and, [3.0 * jnp.abs(w) < points for w in waves])
    squared = waves[0] * waves[0] + waves[1] * waves[1] + waves[2] * waves[2]
    safe_norm = jnp.where(squared > 0, squared, 1.0)
    viscous = squared * (1.0 / points)

    def project(b):
        b = [jnp.where(kept, b[c * PAD : (c + 1) * PAD], 0.0) for c in range(3)]
        along = (waves[0] * b[0] + waves[1] * b[1] + waves[2] * b[2]) / safe_norm
        return [b[c] - waves[c] * along for c in range(3)]

    def tendency(at, re, im):
        joined = grids(
            at,
            jnp.concatenate(re + [-w for w in cross(waves, im)[1:]], 0),
            jnp.concatenate(im + cross(waves, re)[1:], 0))
        fields = [joined[:, c * cell : (c + 1) * cell] for c in range(6)]
        product = jnp.concatenate(cross(fields[:3], fields[3:]), 1)
        b_re, b_im = spectra(at + 2, dot_left(zf, product))
        return (
            [b - viscous * a for b, a in zip(project(b_re), re)],
            [b - viscous * a for b, a in zip(project(b_im), im)],
        )

    b_re, b_im = spectra(0, dot_left(zf, v_ref[...], transposed=True))
    re, im = project(b_re), project(b_im)
    step = 2.0 / points
    r1_re, r1_im = tendency(2, re, im)
    mid_re = [a + step * r for a, r in zip(re, r1_re)]
    mid_im = [a + step * r for a, r in zip(im, r1_im)]
    r2_re, r2_im = tendency(6, mid_re, mid_im)
    end_re = [a + 0.5 * step * (r + s) for a, r, s in zip(re, r1_re, r2_re)]
    end_im = [a + 0.5 * step * (r + s) for a, r, s in zip(im, r1_im, r2_im)]
    out_ref[...] = grids(10, jnp.concatenate(end_re, 0), jnp.concatenate(end_im, 0))


def solution(mesh):
    rows, cols = mesh.shape["row"], mesh.shape["col"]

    def local(velocity):
        points = velocity.shape[3]
        px, py = points // rows, points // cols
        cell, tile = px * py, 2 * px * PAD
        consts = tables(points, rows, cols)
        forward = [(cols, 2 * PAD, 3 * cell), (rows, 3 * PAD, tile)]
        inverse = lambda m, n: [(rows, m * PAD, tile), (cols, n * PAD, 2 * cell)]
        shapes = forward + 2 * (inverse(5, 6) + forward) + inverse(3, 3)
        axes = ["col", "row"] + 2 * ["row", "col", "col", "row"] + ["row", "col"]
        sems = [pltpu.SemaphoreType.DMA(((rows if a == "row" else cols) - 1,)) for a in axes]
        whole = pl.BlockSpec(memory_space=pltpu.VMEM)
        held = [pltpu.VMEM(consts[i].shape, jnp.bfloat16) for i in (2, 4, 5, 3)]
        buffers = [pltpu.VMEM(s, jnp.float32) for s in shapes]
        out = pl.pallas_call(
            functools.partial(kernel, points, rows, cols, axes),
            out_shape=jax.ShapeDtypeStruct((points, 3 * cell), jnp.float32),
            in_specs=[whole] * 3 + [pl.BlockSpec(memory_space=pl.ANY)] * 4 + [whole] * 4,
            out_specs=pl.BlockSpec(memory_space=pltpu.VMEM),
            scratch_shapes=buffers + buffers + sems + sems + held + [pltpu.SemaphoreType.DMA((4,))],
            compiler_params=pltpu.CompilerParams(
                collective_id=0, has_side_effects=True, vmem_limit_bytes=60 * 1024 * 1024),
        )(velocity.reshape(3 * cell, points), *[jnp.asarray(c) for c in consts])
        return out.reshape(points, 3, px, py).transpose(1, 2, 3, 0)

    placed = P(None, "row", "col", None)
    return jax.shard_map(local, mesh=mesh, in_specs=(placed,), out_specs=placed, check_vma=False)
```
